256 devices in a mesh: ens: 4 (over x), zero: 16 (over z, core), cols: 4 (over y).
Axes of the slice: x: 4, y: 4, z: 8, core: 2. Of those that a mesh axis runs over, the one named last changes fastest.
Arguments:
- one_gate: float32 [8192, 8192], P(('ens', 'zero'), 'cols'), parts along dimension 0, may hold values from -0.1875 to 0.1875
- other_gate: float32 [8192, 8192], P(('ens', 'zero'), 'cols'), parts along dimension 0, may hold values from -0.125 to 0.125
- one_up: float32 [8192, 8192], P(('ens', 'zero'), 'cols'), parts along dimension 0, may hold values from -0.1875 to 0.1875
- other_up: float32 [8192, 8192], P(('ens', 'zero'), 'cols'), parts along dimension 0, may hold values from -0.125 to 0.125
- mix_share: float32 [8192], P(('ens', 'zero')), parts along dimension 0, may hold values from 0.2 to 0.8
- norm_train: float32 [8192], P(('ens', 'zero', 'cols')), parts along dimension 0, may hold values from 0.25 to 1.75
- norm_step: float32 [8192], P(('ens', 'zero', 'cols')), parts along dimension 0, may hold values from -0.3 to 0.3
Outputs:
- serve_gate: bfloat16 [8192, 8192], P('ens', 'cols'), parts along dimension 0
- serve_up: bfloat16 [8192, 8192], P('ens', 'cols'), parts along dimension 0
- factor_gate: float32 [32768], P(('ens', 'cols')), parts along dimension 0
- factor_up: float32 [32768], P(('ens', 'cols')), parts along dimension 0
- serve_norm: bfloat16 [8192], P('ens'), parts along dimension 0
The draws below stay inside these ranges and needn't reach their ends.
There are 4 independent parts, one for each index of `ens`. The reference program is written for one: setup_inputs(seed, part) draws one part's arguments, and reference() takes and returns one part's arrays. A program takes and returns all parts, laid end to end along the dimension named above; each array names one. Nothing has to cross between parts.
All inputs are finite; a program needn't handle non-finite values. Where the reference program divides by a largest or mean magnitude, that divisor is 1e-20 or more.
Results may differ from the reference program's by a relative error of at most 0.001.
Values may be sent and summed in bfloat16 or wider, within the bound.
A program may use at most 128 MiB of HBM per device.

```python
import jax
import jax.numpy as jnp

D_MODEL = 2048
D_INNER = 8192


def with_spikes(values, key, source, target, parts, factor):
    owner, partner = [(jnp.arange(values.shape[axis_at]) // (values.shape[axis_at] // parts)).reshape([-1 if axis == axis_at else 1 for axis in range(values.ndim)]) for axis_at in (source, target)]
    chosen = jax.random.permutation(key, parts)[partner]
    strong = (owner == chosen) | (owner == (partner + parts // 2) % parts)
    return jnp.where(strong, factor * values, values)


def levels(rng, extent, split, least, high):
    level = 1.0
    for axis_at, shards_of in split:
        heights = jax.random.uniform(jax.random.fold_in(jax.random.fold_in(rng, 6), axis_at), (shards_of,), jnp.float32, least / len(split), high / len(split))
        level = level * jnp.repeat(jnp.exp(heights), extent[axis_at] // shards_of).reshape((-1,) + (1,) * (len(extent) - 1 - axis_at))
    return level


def centred(stream_key, extent, deviation, bound, cuts=(), held_as=jnp.bfloat16):
    factor_of = levels(stream_key, extent, cuts, -0.22, 0.18) if cuts else 1.0
    entries = jax.random.normal(stream_key, extent, jnp.float32) * deviation * factor_of
    return jnp.minimum(jnp.maximum(entries, -bound), bound).astype(held_as)


def bell_draw_with(rng, extent, scale, limit, split, heavy, held_as=jnp.bfloat16):
    drawn = scale * jax.random.normal(rng, extent, jnp.float32)
    if split:
        drawn = drawn * levels(rng, extent, split, -0.22, 0.18)
    return jnp.clip(with_spikes(drawn, jax.random.fold_in(rng, 3), *heavy), -limit, limit).astype(held_as)


def setup_inputs(seed: int = 0, part: int = 0) -> dict:
    streams_of = jax.random.split(jax.random.key(seed), 8)
    part_splits = jax.random.split(jax.random.fold_in(streams_of[7], part), 8)
    one_gate = bell_draw_with(part_splits[0], (D_MODEL, D_INNER), D_MODEL ** -0.5, 0.1875, ((0, 16), (1, 4)), (0, 1, 16, 2.0), jnp.float32)
    other_gate = centred(part_splits[1], (D_MODEL, D_INNER), D_MODEL ** -0.5, 0.125, ((0, 16), (1, 4)), jnp.float32)
    one_up = bell_draw_with(part_splits[2], (D_MODEL, D_INNER), D_MODEL ** -0.5, 0.1875, ((0, 16), (1, 4)), (0, 1, 16, 2.0), jnp.float32)
    other_up = centred(part_splits[3], (D_MODEL, D_INNER), D_MODEL ** -0.5, 0.125, ((0, 16), (1, 4)), jnp.float32)
    mix_share = jnp.clip(0.2 + 0.6 * jax.random.uniform(part_splits[4], (D_MODEL,), jnp.float32) ** levels(part_splits[4], (D_MODEL,), ((0, 16),), -0.2, 0.2), 0.2, 0.8)
    norm_train = jnp.clip(1.0 + 0.15 * jax.random.normal(part_splits[5], (D_MODEL,), jnp.float32), 0.25, 1.75)
    norm_step = jnp.clip(jax.random.uniform(part_splits[6], (D_MODEL,), jnp.float32, -0.3, 0.3) * levels(part_splits[6], (D_MODEL,), ((0, 64),), -0.4, 0.0), -0.3, 0.3)
    return {"one_gate": one_gate, "other_gate": other_gate, "one_up": one_up, "other_up": other_up, "mix_share": mix_share, "norm_train": norm_train, "norm_step": norm_step}


def reference(one_gate, other_gate, one_up, other_up, mix_share, norm_train, norm_step):
    fresh_gate = mix_share[:, None] * one_gate + (1.0 - mix_share[:, None]) * other_gate
    fresh_up = mix_share[:, None] * one_up + (1.0 - mix_share[:, None]) * other_up
    factor_gate = jnp.sum(jnp.abs(fresh_gate), axis=0) / D_MODEL
    serve_gate = (fresh_gate / factor_gate).astype(jnp.bfloat16)
    factor_up = jnp.sum(jnp.abs(fresh_up), axis=0) / D_MODEL
    serve_up = (fresh_up / factor_up).astype(jnp.bfloat16)
    serve_norm = (norm_train + norm_step).astype(jnp.bfloat16)
    return serve_gate, serve_up, factor_gate, factor_up, serve_norm
```

```python
import jax
import jax.numpy as jnp
from jax import lax
from jax.experimental import pallas as pl
from jax.experimental.pallas import tpu as pltpu
from jax.sharding import PartitionSpec as P

D_MODEL = 2048
MESH = pl.DeviceIdType.MESH
CHIPS = 8
CORES = 2
COLS = 4
PARTS = 2


def gather_kernel(
    one_gate, other_gate, one_up, other_up, mix, norm_train, norm_step,
    out, factor, norm,
    held, mix_rows, sums, paired, chip_sums, norm_cols,
    load_sem, pair_send, pair_recv, sum_send, sum_recv, fac_send, fac_recv,
    col_send, col_recv, nz_send, nz_recv, np_send, np_recv,
    ici_send, ici_recv, die_send, die_recv,
):
    zero = lax.axis_index("zero")
    y = lax.axis_index("cols")
    z, core = zero // CORES, lax.rem(zero, CORES)
    rows, columns = one_gate.shape
    partner = {"zero": z * CORES + 1 - core}
    first, second = 1 - core, core
    half = rows // 2
    size = half // PARTS

    def chip(k):
        return {"zero": lax.rem(z + k, CHIPS) * CORES + core}

    def col(k):
        return {"cols": lax.rem(y + k, COLS)}

    groups = 4
    step = rows // groups

    def load(matrix, which, g):
        source = ((one_gate, other_gate), (one_up, other_up))[matrix][which]
        at = pl.ds(g * step, step)
        return pltpu.make_async_copy(source.at[at], held.at[matrix, which, at], load_sem.at[matrix, which, g])

    def start_loads(matrix):
        for g in range(groups):
            for which in range(2):
                load(matrix, which, g).start()

    @pl.when(core == 0)
    def _():
        start_loads(1)
        start_loads(0)

    @pl.when(core == 1)
    def _():
        start_loads(0)
        start_loads(1)

    barrier = pltpu.get_barrier_semaphore()
    pl.semaphore_signal(barrier, inc=1, device_id=partner, device_id_type=MESH)
    for k in range(1, CHIPS):
        pl.semaphore_signal(barrier, inc=1, device_id=chip(k), device_id_type=MESH)
    for k in range(1, COLS):
        pl.semaphore_signal(barrier, inc=1, device_id=col(k), device_id_type=MESH)

    mix_rows[...] = jnp.broadcast_to(mix[...], (rows, rows)).T
    lane = lax.broadcasted_iota(jnp.int32, (1, 128), 1)
    gain = norm_train[...] + norm_step[...]
    width = gain.shape[1]
    gain = jnp.concatenate([gain] * COLS, axis=1)
    norm_cols[y] = jnp.where((lane >= y * width) & (lane < (y + 1) * width), gain, 0.0)

    def average(matrix):
        total = jnp.zeros((8, columns), jnp.float32)
        for g in range(groups):
            for which in range(2):
                at = pl.ds(g * step, step)
                pltpu.make_async_copy(one_gate.at[at], held.at[matrix, which, at], load_sem.at[matrix, which, g]).wait()

            def body(i, total):
                at = pl.ds(pl.multiple_of(g * step + i * 8, 8), 8)
                share = jnp.concatenate([mix_rows[at]] * (columns // 128), axis=1)
                fresh = share * held[matrix, 0, at] + (1.0 - share) * held[matrix, 1, at]
                held[matrix, 0, at] = fresh
                return total + jnp.abs(fresh)

            total = lax.fori_loop(0, step // 8, body, total)
        sums[matrix] = jnp.sum(total, axis=0, keepdims=True)

    average(first)
    pl.semaphore_wait(barrier, 1 + CHIPS - 1 + COLS - 1)
    pair = pltpu.make_async_remote_copy(
        sums.at[first], paired, pair_send, pair_recv, device_id=partner, device_id_type=MESH
    )
    pair.start()
    col_copies = [
        pltpu.make_async_remote_copy(
            norm_cols.at[y], norm_cols.at[y], col_send.at[k], col_recv.at[k], device_id=col(k), device_id_type=MESH
        )
        for k in range(1, COLS)
    ]
    for copy in col_copies:
        copy.start()
    average(second)
    pair.wait_recv()
    chip_sums[z] = sums[second] + paired[...]
    sum_copies = [
        pltpu.make_async_remote_copy(
            chip_sums.at[z], chip_sums.at[z], sum_send.at[k], sum_recv.at[k], device_id=chip(k), device_id_type=MESH
        )
        for k in (4, 3, 5, 2, 6, 1, 7)
    ]
    for copy in sum_copies:
        copy.start()

    for copy in col_copies:
        copy.wait_recv()
    norm[core, z] = norm_cols[0] + norm_cols[1] + norm_cols[2] + norm_cols[3]
    norm_copies = [
        pltpu.make_async_remote_copy(
            norm.at[core, z], norm.at[core, z], nz_send.at[k], nz_recv.at[k], device_id=chip(k), device_id_type=MESH
        )
        for k in range(1, CHIPS)
    ]

    for copy in sum_copies:
        copy.wait_recv()
    total = chip_sums[0]
    for k in range(1, CHIPS):
        total = total + chip_sums[k]
    mine = total / D_MODEL
    factor[core] = mine
    fac = pltpu.make_async_remote_copy(
        factor.at[core], factor.at[core], fac_send, fac_recv, device_id=partner, device_id_type=MESH
    )
    fac.start()

    def piece(matrix, chip_at, core_at, d, part):
        at = (chip_at * CORES + core_at) * rows + d * half + part * size
        return out.at[matrix, pl.ds(pl.multiple_of(at, size), size)]

    def sign(d):
        return 1 if d == 0 else CHIPS - 1

    def across(d, s, j):
        matrix = core if j < PARTS else 1 - core
        ref = piece(matrix, lax.rem(z + (CHIPS - sign(d)) * s, CHIPS), core, d, j % PARTS)
        return pltpu.make_async_remote_copy(
            ref, ref, ici_send.at[d, s, j], ici_recv.at[d, s, j], device_id=chip(sign(d)), device_id_type=MESH
        )

    def over(d, b, j):
        matrix = core if j < PARTS else 1 - core
        ref = piece(matrix, lax.rem(z + (CHIPS - sign(d)) * b, CHIPS), core, d, j % PARTS)
        return pltpu.make_async_remote_copy(
            ref, ref, die_send.at[d, b, j], die_recv.at[d, b, j], device_id=partner, device_id_type=MESH
        )

    def scale(matrix, inverse, j):
        for d in range(2):
            at = d * half + (j % PARTS) * size
            base = pl.multiple_of(zero * rows + at, size)

            def body(i, _):
                fresh = held[matrix, 0, pl.ds(pl.multiple_of(at + i * 16, 16), 16)]
                out[matrix, pl.ds(pl.multiple_of(base + i * 16, 16), 16)] = (fresh * inverse).astype(jnp.bfloat16)
                return 0

            lax.fori_loop(0, size // 16, body, 0)

    inverse = 1.0 / mine
    for j in range(PARTS):
        scale(second, inverse, j)
        for d in range(2):
            across(d, 0, j).start()
            over(d, 0, j).start()
    for copy in norm_copies:
        copy.start()
    fac.wait_recv()
    inverse = 1.0 / factor[first]
    for j in range(PARTS, 2 * PARTS):
        scale(first, inverse, j)
        for d in range(2):
            across(d, 0, j).start()
            over(d, 0, j).start()

    for copy in norm_copies:
        copy.wait_recv()
    norm_pair = pltpu.make_async_remote_copy(
        norm.at[core], norm.at[core], np_send, np_recv, device_id=partner, device_id_type=MESH
    )
    norm_pair.start()

    def ring(s, _):
        for j in range(2 * PARTS):
            for d in range(2):
                across(d, s, j).wait_recv()

                @pl.when(s < CHIPS - 2)
                def _():
                    across(d, s + 1, j).start()

                over(d, s + 1, j).start()
        return 0

    lax.fori_loop(0, CHIPS - 1, ring, 0)

    pair.wait_send()
    fac.wait_send()
    norm_pair.wait()
    for copy in col_copies + sum_copies + norm_copies:
        copy.wait_send()

    def finish(s, _):
        for j in range(2 * PARTS):
            for d in range(2):
                across(d, s, j).wait_send()
                over(d, s, j).wait()
        return 0

    lax.fori_loop(0, CHIPS - 1, finish, 0)
    for j in range(2 * PARTS):
        for d in range(2):
            over(d, CHIPS - 1, j).wait()


def write_kernel(held, factor, norm, gate, up, factor_gate, factor_up, serve_norm, row, sems):
    copies = []
    pieces = 8
    step = gate.shape[0] // pieces
    for i in range(pieces):
        at = pl.ds(i * step, step)
        copies.append(pltpu.make_async_copy(held.at[0, at], gate.at[at], sems.at[0, i]))
        copies.append(pltpu.make_async_copy(held.at[1, at], up.at[at], sems.at[1, i]))
    copies.append(pltpu.make_async_copy(factor.at[0], factor_gate, sems.at[2, 0]))
    copies.append(pltpu.make_async_copy(factor.at[1], factor_up, sems.at[2, 1]))
    for copy in copies:
        copy.start()
    for i in range(CHIPS):
        for core in range(CORES):
            row[pl.ds(i * CORES + core, 1), :] = norm[core, i]
    serve_norm[...] = row[...].astype(jnp.bfloat16)
    for copy in copies:
        copy.wait()


def local(one_gate, other_gate, one_up, other_up, mix_share, norm_train, norm_step):
    rows, columns = one_gate.shape
    full = CHIPS * CORES * rows
    f32 = jnp.float32
    dma = pltpu.SemaphoreType.DMA
    vmem = pl.BlockSpec(memory_space=pltpu.VMEM)
    hbm = pl.BlockSpec(memory_space=pltpu.HBM)
    one_gate, other_gate, one_up, other_up = (
        pltpu.with_memory_space_constraint(a, pltpu.HBM) for a in (one_gate, other_gate, one_up, other_up)
    )
    held, factor, norm = pl.pallas_call(
        gather_kernel,
        name="gather",
        out_shape=(
            pltpu.VMEM((2, full, columns), jnp.bfloat16),
            pltpu.VMEM((2, 1, columns), f32),
            pltpu.VMEM((CORES, CHIPS, 1, 128), f32),
        ),
        in_specs=[hbm] * 4 + [vmem] * 3,
        out_specs=(vmem, vmem, vmem),
        scratch_shapes=[
            pltpu.VMEM((2, 2, rows, columns), f32),
            pltpu.VMEM((rows, rows), f32),
            pltpu.VMEM((2, 1, columns), f32),
            pltpu.VMEM((1, columns), f32),
            pltpu.VMEM((CHIPS, 1, columns), f32),
            pltpu.VMEM((COLS, 1, 128), f32),
            dma((2, 2, 4)),
            dma, dma,
            dma((CHIPS,)), dma((CHIPS,)),
            dma, dma,
            dma((COLS,)), dma((COLS,)),
            dma((CHIPS,)), dma((CHIPS,)),
            dma, dma,
            dma((2, CHIPS - 1, 2 * PARTS)), dma((2, CHIPS - 1, 2 * PARTS)),
            dma((2, CHIPS, 2 * PARTS)), dma((2, CHIPS, 2 * PARTS)),
        ],
        compiler_params=pltpu.CompilerParams(collective_id=0, has_side_effects=True, vmem_limit_bytes=8 * 2**20),
    )(one_gate, other_gate, one_up, other_up, mix_share.reshape(1, -1), norm_train.reshape(1, -1), norm_step.reshape(1, -1))
    held, factor, norm = (pltpu.with_memory_space_constraint(a, pltpu.VMEM) for a in (held, factor, norm))
    gate, up, factor_gate, factor_up, serve_norm = pl.pallas_call(
        write_kernel,
        name="write",
        out_shape=(
            jax.ShapeDtypeStruct((full, columns), jnp.bfloat16),
            jax.ShapeDtypeStruct((full, columns), jnp.bfloat16),
            jax.ShapeDtypeStruct((1, columns), f32),
            jax.ShapeDtypeStruct((1, columns), f32),
            jax.ShapeDtypeStruct((CHIPS * CORES, 128), jnp.bfloat16),
        ),
        in_specs=[vmem] * 3,
        out_specs=(hbm, hbm, hbm, hbm, vmem),
        scratch_shapes=[pltpu.VMEM((CHIPS * CORES, 128), f32), dma((3, 8))],
        compiler_params=pltpu.CompilerParams(vmem_limit_bytes=2 * 2**20),
    )(held, factor, norm)
    return gate, up, factor_gate.reshape(-1), factor_up.reshape(-1), serve_norm.reshape(-1)


def solution(mesh):
    return jax.shard_map(
        local,
        mesh=mesh,
        in_specs=(
            P(("ens", "zero"), "cols"),
            P(("ens", "zero"), "cols"),
            P(("ens", "zero"), "cols"),
            P(("ens", "zero"), "cols"),
            P(("ens", "zero")),
            P(("ens", "zero", "cols")),
            P(("ens", "zero", "cols")),
        ),
        out_specs=(
            P("ens", "cols"),
            P("ens", "cols"),
            P(("ens", "cols")),
            P(("ens", "cols")),
            P("ens"),
        ),
        check_vma=False,
    )
```

```python
import jax
import jax.numpy as jnp
from jax import lax
from jax.experimental import pallas as pl
from jax.experimental.pallas import tpu as pltpu
from jax.sharding import PartitionSpec as P

D_MODEL = 2048
MESH = pl.DeviceIdType.MESH
CHIPS = 8
CORES = 2
COLS = 4
PARTS = 1


def gather_kernel(
    one_gate, other_gate, one_up, other_up, mix, norm_train, norm_step,
    out, factor, norm,
    held, mix_line, train_line, step_line, mix_rows, sums, paired, chip_sums, norm_cols,
    load_sem, small_sem, pair_send, pair_recv, sum_send, sum_recv, fac_send, fac_recv,
    col_send, col_recv, nz_send, nz_recv, np_send, np_recv,
    ici_send, ici_recv, die_send, die_recv,
):
    zero = lax.axis_index("zero")
    y = lax.axis_index("cols")
    z, core = zero // CORES, lax.rem(zero, CORES)
    rows, columns = one_gate.shape
    partner = {"zero": z * CORES + 1 - core}
    first, second = 1 - core, core
    half = rows // 2
    size = half // PARTS

    def chip(k):
        return {"zero": lax.rem(z + k, CHIPS) * CORES + core}

    def col(k):
        return {"cols": lax.rem(y + k, COLS)}

    groups = 2
    step = rows // groups

    def load(matrix, which, g):
        source = ((one_gate, other_gate), (one_up, other_up))[matrix][which]
        at = pl.ds(g * step, step)
        return pltpu.make_async_copy(source.at[at], held.at[matrix, which, at], load_sem.at[matrix, g])

    def start_loads(matrix):
        for g in range(groups):
            for which in range(2):
                load(matrix, which, g).start()

    small = [
        pltpu.make_async_copy(source, target, small_sem.at[i])
        for i, (source, target) in enumerate(((mix, mix_line), (norm_train, train_line), (norm_step, step_line)))
    ]
    for copy in small:
        copy.start()

    @pl.when(core == 0)
    def _():
        start_loads(1)
        start_loads(0)

    @pl.when(core == 1)
    def _():
        start_loads(0)
        start_loads(1)

    barrier = pltpu.get_barrier_semaphore()
    pl.semaphore_signal(barrier, inc=1, device_id=partner, device_id_type=MESH)
    for k in range(1, CHIPS):
        pl.semaphore_signal(barrier, inc=1, device_id=chip(k), device_id_type=MESH)
    for k in range(1, COLS):
        pl.semaphore_signal(barrier, inc=1, device_id=col(k), device_id_type=MESH)

    for copy in small:
        copy.wait()
    mix_rows[...] = jnp.broadcast_to(mix_line[...], (rows, rows)).T
    lane = lax.broadcasted_iota(jnp.int32, (1, 128), 1)
    gain = train_line[...] + step_line[...]
    width = gain.shape[1]
    gain = jnp.concatenate([gain] * COLS, axis=1)
    norm_cols[y] = jnp.where((lane >= y * width) & (lane < (y + 1) * width), gain, 0.0)

    def arrived(ref, sem):
        pltpu.make_async_copy(ref, ref, sem).wait()

    def average(matrix):
        total = jnp.zeros((8, columns), jnp.float32)
        for g in range(groups):
            landed = held.at[matrix, :, pl.ds(g * step, step)]
            pltpu.make_async_copy(landed, landed, load_sem.at[matrix, g]).wait()

            def body(i, total):
                at = pl.ds(pl.multiple_of(g * step + i * 8, 8), 8)
                share = jnp.concatenate([mix_rows[at]] * (columns // 128), axis=1)
                fresh = share * held[matrix, 0, at] + (1.0 - share) * held[matrix, 1, at]
                held[matrix, 0, at] = fresh
                return total + jnp.abs(fresh)

            total = lax.fori_loop(0, step // 8, body, total)
        sums[matrix] = jnp.sum(total, axis=0, keepdims=True)

    average(first)
    pl.semaphore_wait(barrier, 1 + CHIPS - 1 + COLS - 1)
    pair = pltpu.make_async_remote_copy(
        sums.at[first], paired, pair_send, pair_recv, device_id=partner, device_id_type=MESH
    )
    pair.start()
    col_copies = [
        pltpu.make_async_remote_copy(
            norm_cols.at[y], norm_cols.at[y], col_send, col_recv, device_id=col(k), device_id_type=MESH
        )
        for k in range(1, COLS)
    ]
    for copy in col_copies:
        copy.start()
    average(second)
    pair.wait_recv()
    chip_sums[z] = sums[second] + paired[...]
    sum_copies = [
        pltpu.make_async_remote_copy(
            chip_sums.at[z], chip_sums.at[z], sum_send, sum_recv, device_id=chip(k), device_id_type=MESH
        )
        for k in (4, 3, 5, 2, 6, 1, 7)
    ]
    for copy in sum_copies:
        copy.start()

    arrived(norm_cols.at[pl.ds(0, COLS - 1)], col_recv)
    norm[core, z] = norm_cols[0] + norm_cols[1] + norm_cols[2] + norm_cols[3]
    norm_copies = [
        pltpu.make_async_remote_copy(
            norm.at[core, z], norm.at[core, z], nz_send, nz_recv, device_id=chip(k), device_id_type=MESH
        )
        for k in range(1, CHIPS)
    ]

    arrived(chip_sums.at[pl.ds(0, CHIPS - 1)], sum_recv)
    total = chip_sums[0]
    for k in range(1, CHIPS):
        total = total + chip_sums[k]
    mine = total / D_MODEL
    factor[core] = mine
    fac = pltpu.make_async_remote_copy(
        factor.at[core], factor.at[core], fac_send, fac_recv, device_id=partner, device_id_type=MESH
    )
    fac.start()

    def piece(matrix, chip_at, core_at, d, part):
        at = (chip_at * CORES + core_at) * rows + d * half + part * size
        return out.at[matrix, pl.ds(pl.multiple_of(at, size), size)]

    def sign(d):
        return 1 if d == 0 else CHIPS - 1

    def across(d, s, j):
        matrix = core if j < PARTS else 1 - core
        ref = piece(matrix, lax.rem(z + (CHIPS - sign(d)) * s, CHIPS), core, d, j % PARTS)
        return pltpu.make_async_remote_copy(
            ref, ref, ici_send, ici_recv.at[d, s, j], device_id=chip(sign(d)), device_id_type=MESH
        )

    def over(d, b, j):
        matrix = core if j < PARTS else 1 - core
        ref = piece(matrix, lax.rem(z + (CHIPS - sign(d)) * b, CHIPS), core, d, j % PARTS)
        return pltpu.make_async_remote_copy(
            ref, ref, die_send, die_recv, device_id=partner, device_id_type=MESH
        )

    def scale(matrix, inverse, j):
        for d in range(2):
            at = d * half + (j % PARTS) * size
            base = pl.multiple_of(zero * rows + at, size)

            def body(i, _):
                fresh = held[matrix, 0, pl.ds(pl.multiple_of(at + i * 16, 16), 16)]
                out[matrix, pl.ds(pl.multiple_of(base + i * 16, 16), 16)] = (fresh * inverse).astype(jnp.bfloat16)
                return 0

            lax.fori_loop(0, size // 16, body, 0)

    inverse = 1.0 / mine
    for j in range(PARTS):
        scale(second, inverse, j)
        for d in range(2):
            across(d, 0, j).start()
            over(d, 0, j).start()
    for copy in norm_copies:
        copy.start()
    fac.wait_recv()
    inverse = 1.0 / factor[first]
    for j in range(PARTS, 2 * PARTS):
        scale(first, inverse, j)
        for d in range(2):
            across(d, 0, j).start()
            over(d, 0, j).start()

    arrived(norm.at[core, pl.ds(0, CHIPS - 1)], nz_recv)
    norm_pair = pltpu.make_async_remote_copy(
        norm.at[core], norm.at[core], np_send, np_recv, device_id=partner, device_id_type=MESH
    )
    norm_pair.start()

    def ring(s, _):
        for j in range(2 * PARTS):
            for d in range(2):
                across(d, s, j).wait_recv()

                @pl.when(s < CHIPS - 2)
                def _():
                    across(d, s + 1, j).start()

                over(d, s + 1, j).start()
        return 0

    lax.fori_loop(0, CHIPS - 1, ring, 0)

    pair.wait_send()
    fac.wait_send()
    norm_pair.wait()
    arrived(norm_cols.at[pl.ds(0, COLS - 1)], col_send)
    arrived(chip_sums.at[pl.ds(0, CHIPS - 1)], sum_send)
    arrived(norm.at[core, pl.ds(0, CHIPS - 1)], nz_send)
    arrived(out.at[0, pl.ds(0, 2 * (CHIPS - 1) * rows)], ici_send)
    arrived(out.at[0], die_send)
    arrived(out.at[0], die_recv)


def write_kernel(held, factor, norm, gate, up, factor_gate, factor_up, serve_norm, row, line, sems):
    pieces = 16
    step = gate.shape[0] // pieces
    for i in range(pieces):
        for matrix, target in enumerate((gate, up)):
            at = pl.ds(i * step, step)
            pltpu.make_async_copy(held.at[matrix, at], target.at[at], sems.at[matrix]).start()
    factors = [
        pltpu.make_async_copy(factor.at[matrix], target, sems.at[2 + matrix])
        for matrix, target in enumerate((factor_gate, factor_up))
    ]
    for copy in factors:
        copy.start()
    for i in range(CHIPS):
        for core in range(CORES):
            row[pl.ds(i * CORES + core, 1), :] = norm[core, i]
    line[...] = row[...].astype(jnp.bfloat16)
    last = pltpu.make_async_copy(line, serve_norm, sems.at[4])
    last.start()
    for copy in factors:
        copy.wait()
    for matrix, target in enumerate((gate, up)):
        pltpu.make_async_copy(held.at[matrix], target, sems.at[matrix]).wait()
    last.wait()


def local(one_gate, other_gate, one_up, other_up, mix_share, norm_train, norm_step):
    rows, columns = one_gate.shape
    full = CHIPS * CORES * rows
    f32 = jnp.float32
    dma = pltpu.SemaphoreType.DMA
    vmem = pl.BlockSpec(memory_space=pltpu.VMEM)
    hbm = pl.BlockSpec(memory_space=pltpu.HBM)
    taken = [
        pltpu.with_memory_space_constraint(a, pltpu.HBM)
        for a in (
            one_gate, other_gate, one_up, other_up,
            mix_share.reshape(1, -1), norm_train.reshape(1, -1), norm_step.reshape(1, -1),
        )
    ]
    held, factor, norm = pl.pallas_call(
        gather_kernel,
        name="gather",
        out_shape=(
            pltpu.VMEM((2, full, columns), jnp.bfloat16),
            pltpu.VMEM((2, 1, columns), f32),
            pltpu.VMEM((CORES, CHIPS, 1, 128), f32),
        ),
        in_specs=[hbm] * 7,
        out_specs=(vmem, vmem, vmem),
        scratch_shapes=[
            pltpu.VMEM((2, 2, rows, columns), f32),
            pltpu.VMEM((1, rows), f32),
            pltpu.VMEM((1, norm_train.size), f32),
            pltpu.VMEM((1, norm_train.size), f32),
            pltpu.VMEM((rows, rows), f32),
            pltpu.VMEM((2, 1, columns), f32),
            pltpu.VMEM((1, columns), f32),
            pltpu.VMEM((CHIPS, 1, columns), f32),
            pltpu.VMEM((COLS, 1, 128), f32),
            dma((2, 2)), dma((3,)),
            dma, dma, dma, dma, dma, dma,
            dma, dma, dma, dma, dma, dma,
            dma, dma((2, CHIPS - 1, 2 * PARTS)), dma, dma,
        ],
        compiler_params=pltpu.CompilerParams(collective_id=0, has_side_effects=True, vmem_limit_bytes=8 * 2**20),
    )(*taken)
    held, factor, norm = (pltpu.with_memory_space_constraint(a, pltpu.VMEM) for a in (held, factor, norm))
    gate, up, factor_gate, factor_up, serve_norm = pl.pallas_call(
        write_kernel,
        name="write",
        out_shape=(
            jax.ShapeDtypeStruct((full, columns), jnp.bfloat16),
            jax.ShapeDtypeStruct((full, columns), jnp.bfloat16),
            jax.ShapeDtypeStruct((1, columns), f32),
            jax.ShapeDtypeStruct((1, columns), f32),
            jax.ShapeDtypeStruct((CHIPS * CORES, 128), jnp.bfloat16),
        ),
        in_specs=[vmem] * 3,
        out_specs=(hbm,) * 5,
        scratch_shapes=[pltpu.VMEM((CHIPS * CORES, 128), f32), pltpu.VMEM((CHIPS * CORES, 128), jnp.bfloat16), dma((5,))],
        compiler_params=pltpu.CompilerParams(vmem_limit_bytes=2 * 2**20),
    )(held, factor, norm)
    return gate, up, factor_gate.reshape(-1), factor_up.reshape(-1), serve_norm.reshape(-1)


def solution(mesh):
    return jax.shard_map(
        local,
        mesh=mesh,
        in_specs=(
            P(("ens", "zero"), "cols"),
            P(("ens", "zero"), "cols"),
            P(("ens", "zero"), "cols"),
            P(("ens", "zero"), "cols"),
            P(("ens", "zero")),
            P(("ens", "zero", "cols")),
            P(("ens", "zero", "cols")),
        ),
        out_specs=(
            P("ens", "cols"),
            P("ens", "cols"),
            P(("ens", "cols")),
            P(("ens", "cols")),
            P("ens"),
        ),
        check_vma=False,
    )
```

```python
import jax
import jax.numpy as jnp
from jax import lax
from jax.experimental import pallas as pl
from jax.experimental.pallas import tpu as pltpu
from jax.sharding import PartitionSpec as P

D_MODEL = 2048
MESH = pl.DeviceIdType.MESH
CHIPS = 8
CORES = 2
COLS = 4
PARTS = 2
EARLY = (8, 16)


def gather_kernel(
    one_gate, other_gate, one_up, other_up, mix, norm_train, norm_step,
    out, factor, norm,
    held, early, mix_line, train_line, step_line, mix_rows, sums, paired, chip_sums, norm_cols,
    load_sem, small_sem, pair_send, pair_recv, sum_send, sum_recv, fac_send, fac_recv,
    col_send, col_recv, nz_send, nz_recv, np_send, np_recv,
    early_send, early_recv, ici_send, ici_recv, die_send, die_recv,
):
    zero = lax.axis_index("zero")
    y = lax.axis_index("cols")
    z, core = zero // CORES, lax.rem(zero, CORES)
    rows, columns = one_gate.shape
    partner = {"zero": z * CORES + 1 - core}
    first, second = 1 - core, core
    half = rows // 2
    size = half // PARTS

    def chip(k):
        return {"zero": lax.rem(z + k, CHIPS) * CORES + core}

    def sign(d):
        return 1 if d == 0 else CHIPS - 1

    def col(k):
        return {"cols": lax.rem(y + k, COLS)}

    groups = 2
    step = rows // groups

    def load(matrix, which, g):
        source = ((one_gate, other_gate), (one_up, other_up))[matrix][which]
        at = pl.ds(g * step, step)
        return pltpu.make_async_copy(source.at[at], held.at[matrix, which, at], load_sem.at[matrix, g])

    def start_loads(matrix):
        for g in range(groups):
            for which in range(2):
                load(matrix, which, g).start()

    small = [
        pltpu.make_async_copy(source, target, small_sem.at[i])
        for i, (source, target) in enumerate(((mix, mix_line), (norm_train, train_line), (norm_step, step_line)))
    ]
    for copy in small:
        copy.start()

    @pl.when(core == 0)
    def _():
        start_loads(1)
        start_loads(0)

    @pl.when(core == 1)
    def _():
        start_loads(0)
        start_loads(1)

    barrier = pltpu.get_barrier_semaphore()
    pl.semaphore_signal(barrier, inc=1, device_id=partner, device_id_type=MESH)
    for k in range(1, CHIPS):
        pl.semaphore_signal(barrier, inc=1, device_id=chip(k), device_id_type=MESH)
    for k in range(1, COLS):
        pl.semaphore_signal(barrier, inc=1, device_id=col(k), device_id_type=MESH)

    for copy in small:
        copy.wait()
    mix_rows[...] = jnp.broadcast_to(mix_line[...], (rows, rows)).T
    lane = lax.broadcasted_iota(jnp.int32, (1, 128), 1)
    gain = train_line[...] + step_line[...]
    width = gain.shape[1]
    gain = jnp.concatenate([gain] * COLS, axis=1)
    norm_cols[y] = jnp.where((lane >= y * width) & (lane < (y + 1) * width), gain, 0.0)

    def arrived(ref, sem):
        pltpu.make_async_copy(ref, ref, sem).wait()

    def average(matrix):
        total = jnp.zeros((8, columns), jnp.float32)
        for g in range(groups):
            landed = held.at[matrix, :, pl.ds(g * step, step)]
            pltpu.make_async_copy(landed, landed, load_sem.at[matrix, g]).wait()

            def body(i, total):
                at = pl.ds(pl.multiple_of(g * step + i * 8, 8), 8)
                share = jnp.concatenate([mix_rows[at]] * (columns // 128), axis=1)
                fresh = share * held[matrix, 0, at] + (1.0 - share) * held[matrix, 1, at]
                held[matrix, 0, at] = fresh
                return total + jnp.abs(fresh)

            total = lax.fori_loop(0, step // 8, body, total)
        sums[matrix] = jnp.sum(total, axis=0, keepdims=True)

    average(first)
    pl.semaphore_wait(barrier, 1 + CHIPS - 1 + COLS - 1)
    pair = pltpu.make_async_remote_copy(
        sums.at[first], paired, pair_send, pair_recv, device_id=partner, device_id_type=MESH
    )
    pair.start()
    col_copies = [
        pltpu.make_async_remote_copy(
            norm_cols.at[y], norm_cols.at[y], col_send, col_recv, device_id=col(k), device_id_type=MESH
        )
        for k in range(1, COLS)
    ]
    for copy in col_copies:
        copy.start()

    def ahead(i, d):
        start = (0, EARLY[0])[i]
        at = pl.ds(d * half + start, EARLY[i] - start)
        return pltpu.make_async_remote_copy(
            held.at[first, 0, at],
            early.at[d, pl.ds(start, EARLY[i] - start)],
            early_send,
            early_recv,
            device_id=chip(sign(d)),
            device_id_type=MESH,
        )

    if EARLY[0]:
        for d in range(2):
            ahead(0, d).start()
    average(second)
    pair.wait_recv()
    chip_sums[z] = sums[second] + paired[...]
    sum_copies = [
        pltpu.make_async_remote_copy(
            chip_sums.at[z], chip_sums.at[z], sum_send, sum_recv, device_id=chip(k), device_id_type=MESH
        )
        for k in (4, 3, 5, 2, 6, 1, 7)
    ]
    for copy in sum_copies:
        copy.start()
    if EARLY[1] > EARLY[0]:
        for d in range(2):
            ahead(1, d).start()

    arrived(norm_cols.at[pl.ds(0, COLS - 1)], col_recv)
    norm[core, z] = norm_cols[0] + norm_cols[1] + norm_cols[2] + norm_cols[3]
    norm_copies = [
        pltpu.make_async_remote_copy(
            norm.at[core, z], norm.at[core, z], nz_send, nz_recv, device_id=chip(k), device_id_type=MESH
        )
        for k in range(1, CHIPS)
    ]

    arrived(chip_sums.at[pl.ds(0, CHIPS - 1)], sum_recv)
    total = chip_sums[0]
    for k in range(1, CHIPS):
        total = total + chip_sums[k]
    mine = total / D_MODEL
    factor[core] = mine
    fac = pltpu.make_async_remote_copy(
        factor.at[core], factor.at[core], fac_send, fac_recv, device_id=partner, device_id_type=MESH
    )
    fac.start()

    def piece(matrix, chip_at, core_at, d, part):
        at = (chip_at * CORES + core_at) * rows + d * half + part * size
        return out.at[matrix, pl.ds(pl.multiple_of(at, size), size)]

    def across(d, s, j, skip=0):
        matrix = core if j < PARTS else 1 - core
        ref = piece(matrix, lax.rem(z + (CHIPS - sign(d)) * s, CHIPS), core, d, j % PARTS)
        if skip:
            ref = ref.at[pl.ds(skip, size - skip)]
        return pltpu.make_async_remote_copy(
            ref, ref, ici_send, ici_recv.at[d, s, j], device_id=chip(sign(d)), device_id_type=MESH
        )

    def over(d, b, j):
        matrix = core if j < PARTS else 1 - core
        ref = piece(matrix, lax.rem(z + (CHIPS - sign(d)) * b, CHIPS), core, d, j % PARTS)
        return pltpu.make_async_remote_copy(
            ref, ref, die_send, die_recv, device_id=partner, device_id_type=MESH
        )

    def narrow(source, target, count, inverse):
        def body(i, _):
            at = pl.ds(pl.multiple_of(i * 8, 8), 8)
            target[at] = (source[at] * inverse).astype(jnp.bfloat16)
            return 0

        lax.fori_loop(0, count // 8, body, 0)

    def scale(matrix, inverse, j):
        for d in range(2):
            at = pl.ds(d * half + (j % PARTS) * size, size)
            narrow(held.at[matrix, 0, at], piece(matrix, z, core, d, j % PARTS), size, inverse)

    inverse = 1.0 / mine
    for j in range(PARTS):
        scale(second, inverse, j)
        for d in range(2):
            across(d, 0, j).start()
            over(d, 0, j).start()
    for copy in norm_copies:
        copy.start()
    fac.wait_recv()
    inverse = 1.0 / factor[first]
    for j in range(PARTS, 2 * PARTS):
        scale(first, inverse, j)
        for d in range(2):
            across(d, 0, j, EARLY[1] if j == PARTS else 0).start()
            over(d, 0, j).start()
    arrived(early.at[:, pl.ds(0, EARLY[1])], early_recv)
    for d in range(2):
        narrow(early.at[d], piece(first, lax.rem(z + CHIPS - sign(d), CHIPS), core, d, 0), EARLY[1], inverse)

    arrived(norm.at[core, pl.ds(0, CHIPS - 1)], nz_recv)
    norm_pair = pltpu.make_async_remote_copy(
        norm.at[core], norm.at[core], np_send, np_recv, device_id=partner, device_id_type=MESH
    )
    norm_pair.start()

    def ring(s, _, first_step=False):
        for j in range(2 * PARTS):
            for d in range(2):
                across(d, s, j, EARLY[1] if first_step and j == PARTS else 0).wait_recv()

                @pl.when(s < CHIPS - 2)
                def _():
                    across(d, s + 1, j).start()

                over(d, s + 1, j).start()
        return 0

    ring(0, 0, True)
    lax.fori_loop(1, CHIPS - 1, ring, 0)

    pair.wait_send()
    fac.wait_send()
    norm_pair.wait()
    arrived(norm_cols.at[pl.ds(0, COLS - 1)], col_send)
    arrived(chip_sums.at[pl.ds(0, CHIPS - 1)], sum_send)
    arrived(norm.at[core, pl.ds(0, CHIPS - 1)], nz_send)
    arrived(early.at[:, pl.ds(0, EARLY[1])], early_send)
    arrived(out.at[0, pl.ds(0, 2 * (CHIPS - 1) * rows - 2 * EARLY[1])], ici_send)
    arrived(out.at[0], die_send)
    arrived(out.at[0], die_recv)


def write_kernel(held, factor, norm, gate, up, factor_gate, factor_up, serve_norm, row, line, sems):
    pieces = 16
    step = gate.shape[0] // pieces
    for i in range(pieces):
        for matrix, target in enumerate((gate, up)):
            at = pl.ds(i * step, step)
            pltpu.make_async_copy(held.at[matrix, at], target.at[at], sems.at[matrix]).start()
    factors = [
        pltpu.make_async_copy(factor.at[matrix], target, sems.at[2 + matrix])
        for matrix, target in enumerate((factor_gate, factor_up))
    ]
    for copy in factors:
        copy.start()
    for i in range(CHIPS):
        for core in range(CORES):
            row[pl.ds(i * CORES + core, 1), :] = norm[core, i]
    line[...] = row[...].astype(jnp.bfloat16)
    last = pltpu.make_async_copy(line, serve_norm, sems.at[4])
    last.start()
    for copy in factors:
        copy.wait()
    for matrix, target in enumerate((gate, up)):
        pltpu.make_async_copy(held.at[matrix], target, sems.at[matrix]).wait()
    last.wait()


def local(one_gate, other_gate, one_up, other_up, mix_share, norm_train, norm_step):
    rows, columns = one_gate.shape
    full = CHIPS * CORES * rows
    f32 = jnp.float32
    dma = pltpu.SemaphoreType.DMA
    vmem = pl.BlockSpec(memory_space=pltpu.VMEM)
    hbm = pl.BlockSpec(memory_space=pltpu.HBM)
    taken = [
        pltpu.with_memory_space_constraint(a, pltpu.HBM)
        for a in (
            one_gate, other_gate, one_up, other_up,
            mix_share.reshape(1, -1), norm_train.reshape(1, -1), norm_step.reshape(1, -1),
        )
    ]
    held, factor, norm = pl.pallas_call(
        gather_kernel,
        name="gather",
        out_shape=(
            pltpu.VMEM((2, full, columns), jnp.bfloat16),
            pltpu.VMEM((2, 1, columns), f32),
            pltpu.VMEM((CORES, CHIPS, 1, 128), f32),
        ),
        in_specs=[hbm] * 7,
        out_specs=(vmem, vmem, vmem),
        scratch_shapes=[
            pltpu.VMEM((2, 2, rows, columns), f32),
            pltpu.VMEM((2, rows // 4, columns), f32),
            pltpu.VMEM((1, rows), f32),
            pltpu.VMEM((1, norm_train.size), f32),
            pltpu.VMEM((1, norm_train.size), f32),
            pltpu.VMEM((rows, rows), f32),
            pltpu.VMEM((2, 1, columns), f32),
            pltpu.VMEM((1, columns), f32),
            pltpu.VMEM((CHIPS, 1, columns), f32),
            pltpu.VMEM((COLS, 1, 128), f32),
            dma((2, 2)), dma((3,)),
            dma, dma, dma, dma, dma, dma,
            dma, dma, dma, dma, dma, dma,
            dma, dma, dma, dma((2, CHIPS - 1, 2 * PARTS)), dma, dma,
        ],
        compiler_params=pltpu.CompilerParams(collective_id=0, has_side_effects=True, vmem_limit_bytes=8 * 2**20),
    )(*taken)
    held, factor, norm = (pltpu.with_memory_space_constraint(a, pltpu.VMEM) for a in (held, factor, norm))
    gate, up, factor_gate, factor_up, serve_norm = pl.pallas_call(
        write_kernel,
        name="write",
        out_shape=(
            jax.ShapeDtypeStruct((full, columns), jnp.bfloat16),
            jax.ShapeDtypeStruct((full, columns), jnp.bfloat16),
            jax.ShapeDtypeStruct((1, columns), f32),
            jax.ShapeDtypeStruct((1, columns), f32),
            jax.ShapeDtypeStruct((CHIPS * CORES, 128), jnp.bfloat16),
        ),
        in_specs=[vmem] * 3,
        out_specs=(hbm,) * 5,
        scratch_shapes=[pltpu.VMEM((CHIPS * CORES, 128), f32), pltpu.VMEM((CHIPS * CORES, 128), jnp.bfloat16), dma((5,))],
        compiler_params=pltpu.CompilerParams(vmem_limit_bytes=2 * 2**20),
    )(held, factor, norm)
    return gate, up, factor_gate.reshape(-1), factor_up.reshape(-1), serve_norm.reshape(-1)


def solution(mesh):
    return jax.shard_map(
        local,
        mesh=mesh,
        in_specs=(
            P(("ens", "zero"), "cols"),
            P(("ens", "zero"), "cols"),
            P(("ens", "zero"), "cols"),
            P(("ens", "zero"), "cols"),
            P(("ens", "zero")),
            P(("ens", "zero", "cols")),
            P(("ens", "zero", "cols")),
        ),
        out_specs=(
            P("ens", "cols"),
            P("ens", "cols"),
            P(("ens", "cols")),
            P(("ens", "cols")),
            P("ens"),
        ),
        check_vma=False,
    )
```
